32 devices in a mesh: dp: 4 (over y, x), expert: 8 (over z, core).
Axes of the slice: x: 2, y: 2, z: 4, core: 2. Of those that a mesh axis runs over, the one named last changes fastest.
Arguments:
- out_grad: bfloat16 [384, 3072], P(('dp', 'expert')), may hold values from -6 to 6
- layer_input: bfloat16 [384, 3072], P(('dp', 'expert')), may hold values from -6 to 6
- expert_ids: int32 [384, 2], P(('dp', 'expert')), may hold values from 0 to 7, as said below
- gate_prob: float32 [384, 2], P(('dp', 'expert')), may hold values from 0.05 to 1
- w_stack: bfloat16 [3, 3072, 8192], P(None, 'dp', 'expert'), may hold values from -0.109375 to 0.109375
- scale_exps: int32 [3, 24, 64], P(None, 'dp', 'expert'), may hold values from -1 to 1
Outputs:
- input_grad: bfloat16 [384, 3072], P(('dp', 'expert'))
- weight_grads: float32 [3, 3072, 8192], P(None, 'dp', 'expert')
The draws below stay inside these ranges and needn't reach their ends.
Inputs may be any that keep to these rules, and one draw needn't show every extreme that they name: `expert_ids`: each row names two different experts. In each aligned block of 12 rows (the tokens of one device) between 1 and 3 rows name expert 0, and some blocks have exactly 3 in every draw.
All inputs are finite; a program needn't handle non-finite values.
Results may differ from the reference program's by a relative error of at most 0.015.
Values may be sent and summed in bfloat16 or wider, within the bound.
A program may use at most 128 MiB of HBM per device.

```python
import math
import jax
import jax.numpy as jnp
from jax import lax

D = 3072
FF = 8192
EXPERTS = 8
TOP = 2
TILE = 128
CAP = 3
TOK_DEV = 12
TOKENS = 384
N_DP = 4
N_EXPERT = 8


def draw_expert_ids(key, part):
    block_count = TOKENS // TOK_DEV
    subkeys = jax.random.split(jax.random.fold_in(key, 11), 7)
    counts = jax.random.randint(subkeys[0], (block_count,), 1, CAP + 1)
    full_block = jax.random.randint(subkeys[1], (block_count,), 0, 4) == 0
    chosen = jax.random.randint(subkeys[2], (), 0, block_count)
    counts = jnp.where(full_block | (jnp.arange(block_count) == chosen), CAP, counts)
    ranks = jax.vmap(lambda subkey: jax.random.permutation(subkey, TOK_DEV))(jax.random.split(subkeys[3], block_count))
    routed = ranks < counts[:, None]
    first_pick = jax.random.randint(subkeys[4], (block_count, TOK_DEV), 1, EXPERTS)
    offset = jax.random.randint(subkeys[5], (block_count, TOK_DEV), 1, EXPERTS - 1)
    second = 1 + (first_pick - 1 + offset) % (EXPERTS - 1)
    flipped = jax.random.randint(subkeys[6], (block_count, TOK_DEV), 0, 2) == 1
    column_left = jnp.where(routed, jnp.where(flipped, first_pick, 0), first_pick)
    column_right = jnp.where(routed, jnp.where(flipped, 0, first_pick), second)
    return jnp.stack([column_left, column_right], axis=-1).reshape(TOKENS, 2).astype(jnp.int32)


def with_ends(entries, stream_key, low, high):
    longest = entries.shape.index(max(entries.shape))
    spots = []
    for shift in (0, 1):
        where = [jax.random.randint(jax.random.fold_in(stream_key, axis), (), 0, length) for axis, length in enumerate(entries.shape)]
        where[longest] = (where[longest] + shift) % entries.shape[longest]
        spots.append(tuple(where))
    return entries.at[spots[0]].set(low).at[spots[1]].set(high)


def levels(rng, shape, cuts, low, high):
    def one(axis_at, parts):
        steps = jax.random.uniform(jax.random.fold_in(jax.random.fold_in(rng, 6), axis_at), (parts,), jnp.float32, low / len(cuts), high / len(cuts))
        return jnp.repeat(jnp.exp(steps), shape[axis_at] // parts).reshape((-1,) + (1,) * (len(shape) - axis_at - 1))

    loudness = one(*cuts[0])
    for cut in cuts[1:]:
        loudness = loudness * one(*cut)
    return loudness


def scatter_about(stream_key, dims, deviation, limit, pieces=(), kind=jnp.bfloat16):
    drawn = jax.random.normal(stream_key, dims, jnp.float32) * deviation
    if len(pieces) > 0:
        drawn = levels(stream_key, dims, pieces, -0.22, 0.18) * drawn
    return jnp.clip(drawn, min=-limit, max=limit).astype(kind)


def setup_inputs(seed: int = 0) -> dict:
    key_list = jax.random.split(jax.random.key(seed), 7)
    return {
        "out_grad": scatter_about(key_list[0], (TOKENS, D), 1.0, 6.0, ((0, 32),)),
        "layer_input": scatter_about(key_list[1], (TOKENS, D), 1.0, 6.0, ((0, 32),)),
        "expert_ids": draw_expert_ids(jax.random.fold_in(key_list[6], 71), 0),
        "gate_prob": jnp.clip(jnp.exp(math.log(1.0) - 2.9957323 * jax.random.uniform(key_list[3], (TOKENS, TOP), jnp.float32) ** levels(key_list[3], (TOKENS, TOP), ((0, 32),), -0.2, 0.2)), 0.05, 1.0),
        "w_stack": scatter_about(key_list[4], (3, D, FF), D ** -0.5, 0.109375, ((1, 4), (2, 8))),
        "scale_exps": with_ends(jax.random.randint(key_list[5], (3, D // TILE, FF // TILE), -1, 2), jax.random.fold_in(key_list[5], 1), -1, 1).astype(jnp.int32),
    }


def dequantize(w_stack, scale_exps):
    factor = jnp.exp2(scale_exps.astype(jnp.float32))
    scaled = w_stack.astype(jnp.float32).reshape(3, D // TILE, TILE, FF // TILE, TILE) * factor[:, :, None, :, None]
    return scaled.reshape(3, D, FF).astype(jnp.bfloat16)


def contract_rows(left, right):
    return lax.dot_general(left, right, (((0,), (0,)), ((), ())), preferred_element_type=jnp.float32)


def back_project(grad_rows, matrix):
    return lax.dot_general(grad_rows, matrix, (((1,), (1,)), ((), ())), preferred_element_type=jnp.float32)


def expert_backward(routed_input, routed_grad, weights):
    gate_value = jnp.dot(routed_input, weights[0], preferred_element_type=jnp.float32)
    up_value = jnp.dot(routed_input, weights[1], preferred_element_type=jnp.float32)
    down_back = jnp.dot(routed_grad, weights[2], preferred_element_type=jnp.float32)
    gate_sigmoid = jax.nn.sigmoid(gate_value)
    gate_act = gate_value * gate_sigmoid
    gate_grad = (down_back * up_value * gate_sigmoid * (1.0 + gate_value * (1.0 - gate_sigmoid))).astype(jnp.bfloat16)
    up_grad = (down_back * gate_act).astype(jnp.bfloat16)
    hidden = (gate_act * up_value).astype(jnp.bfloat16)
    returned = back_project(gate_grad, weights[0]) + back_project(up_grad, weights[1])
    partial_value = jnp.stack([contract_rows(routed_input, gate_grad), contract_rows(routed_input, up_grad), contract_rows(routed_grad, hidden)])
    return returned, partial_value


def reference(out_grad, layer_input, expert_ids, gate_prob, w_stack, scale_exps):
    weights = dequantize(w_stack, scale_exps)
    routed = expert_ids == 0
    routed_mask = jnp.any(routed, axis=1)
    expert_prob = jnp.sum(jnp.where(routed, gate_prob, 0.0), axis=1)
    block_count = out_grad.shape[0] // TOK_DEV
    block_mask = routed_mask.reshape(block_count, TOK_DEV)
    slot_index = jnp.cumsum(block_mask.astype(jnp.int32), axis=1) - 1
    places = jnp.arange(CAP, dtype=jnp.int32)
    slot_hit = (slot_index[:, None, :] == places[None, :, None]) & block_mask[:, None, :]
    positions = jnp.arange(TOK_DEV, dtype=jnp.int32)
    source = jnp.sum(jnp.where(slot_hit, positions[None, None, :], 0), axis=2)
    source = (source + (jnp.arange(block_count, dtype=jnp.int32) * TOK_DEV)[:, None]).reshape(-1)
    slot_valid = jnp.any(slot_hit, axis=2).reshape(-1)
    slot_input = jnp.where(slot_valid[:, None], layer_input[source], jnp.zeros((), jnp.bfloat16))
    slot_grad = jnp.where(slot_valid[:, None], expert_prob[source][:, None] * out_grad[source].astype(jnp.float32), 0.0).astype(jnp.bfloat16)
    slot_rows = N_EXPERT * CAP
    group_input = slot_input.reshape(N_DP, slot_rows, D)
    group_grad = slot_grad.reshape(N_DP, slot_rows, D)

    def group_step(total, pair):
        returned, partial_value = expert_backward(pair[0], pair[1], weights)
        rounded = lax.optimization_barrier(partial_value.astype(jnp.bfloat16))
        return total + rounded.astype(jnp.float32), returned

    weight_grads, returned = lax.scan(group_step, jnp.zeros((3, D, FF), jnp.float32), (group_input, group_grad))
    returned = returned.reshape(block_count, CAP, D)
    picked = jnp.take_along_axis(returned, jnp.clip(slot_index, 0, CAP - 1)[:, :, None], axis=1)
    input_grad = jnp.where(block_mask[:, :, None], picked, 0.0).reshape(-1, D).astype(jnp.bfloat16)
    return input_grad, weight_grads
```

```python
import functools

import jax
import jax.numpy as jnp
from jax import lax
from jax.experimental import pallas as pl
from jax.experimental.pallas import tpu as pltpu
from jax.sharding import PartitionSpec as P

TILE = 128
CAP = 3
BF = jnp.bfloat16
F32 = jnp.float32
VMEM_LIMIT = 60 * 1024 * 1024


def iota(shape, dim):
    return lax.broadcasted_iota(jnp.int32, shape, dim)


def mm(a, b, ca=1, cb=0):
    return lax.dot_general(a, b, (((ca,), (cb,)), ((), ())), preferred_element_type=F32)


def exchange_kernel(
    n_dp, n_ex, chunk,
    og_ref, li_ref, ids_ref, prob_ref, exps_ref, w_hbm,
    xt_ref, act_ref, ig_ref,
    w, slab_out, slabs, x, part_out, part_in, acts, acc, back_out, back_in, own_out, own_in,
    w_sem, s1_send, s1_recv, s2_send, s2_recv, s3_send, s3_recv, rs_send, rs_recv,
    ag_send, ag_recv, b1_send, b1_recv, b2_send, b2_recv,
):
    p, e = lax.axis_index("dp"), lax.axis_index("expert")
    tok, width = og_ref.shape
    _, depth, hid = w.shape
    rows = n_ex * CAP
    n_chunk = hid // chunk
    pairs = n_ex // 2
    z, core = e // 2, e % 2
    partner = 2 * z + 1 - core

    def send(src, dst, ssem, rsem, q, f):
        copy = pltpu.make_async_remote_copy(
            src_ref=src, dst_ref=dst, send_sem=ssem, recv_sem=rsem,
            device_id=(q, f), device_id_type=pl.DeviceIdType.MESH,
        )
        copy.start()
        return copy

    w_copies = [
        pltpu.make_async_copy(w_hbm.at[m], w.at[m], w_sem.at[m]) for m in range(3)
    ]
    for copy in w_copies:
        copy.start()

    barrier = pltpu.get_barrier_semaphore()
    for k in range(1, n_dp):
        pl.semaphore_signal(
            barrier, inc=1, device_id=(lax.rem(p + k, n_dp), e),
            device_id_type=pl.DeviceIdType.MESH,
        )
    for k in range(1, n_ex):
        pl.semaphore_signal(
            barrier, inc=1, device_id=(p, lax.rem(e + k, n_ex)),
            device_id_type=pl.DeviceIdType.MESH,
        )

    routed = ids_ref[...] == 0
    mask = jnp.max(routed.astype(F32), axis=1, keepdims=True)
    prob = jnp.sum(jnp.where(routed, prob_ref[...], 0.0), axis=1, keepdims=True)
    earlier = (iota((tok, tok), 1) <= iota((tok, tok), 0)).astype(F32)
    mask_wide = jnp.broadcast_to(mask, (tok, 128))
    place = mm(earlier, mask_wide) - 1.0
    lane = iota((tok, 128), 1).astype(F32)
    hit_in = jnp.where((place == lane) & (mask_wide > 0.5), 1.0, 0.0)
    hit_gr = jnp.where((place + CAP == lane) & (mask_wide > 0.5), 1.0, 0.0)
    scaled = (og_ref[...].astype(F32) * prob).astype(BF)
    slots = (
        mm(hit_in[:, :8].astype(BF), li_ref[...], 0, 0)
        + mm(hit_gr[:, :8].astype(BF), scaled, 0, 0)
    ).astype(BF)
    for q in range(n_dp):
        slab_out[q] = slots[:, q * depth:(q + 1) * depth]
    pl.semaphore_wait(barrier, n_dp - 1 + n_ex - 1)

    pend = []
    for k in range(1, n_dp):
        q = lax.rem(p + k, n_dp)
        pend.append(send(slab_out.at[q], slabs.at[e, p], s1_send.at[k], s1_recv.at[k], q, e))
    slabs[e, p] = slab_out[p]
    for copy in pend:
        copy.wait()

    pend = [send(slabs.at[e], slabs.at[e], s2_send.at[0], s2_recv.at[0], p, partner)]
    for k in range(1, pairs):
        f = 2 * lax.rem(z + k, pairs) + core
        pend.append(send(slabs.at[e], slabs.at[e], s2_send.at[k], s2_recv.at[k], p, f))

    for copy in w_copies:
        copy.wait()
    tr, tc = depth // TILE, hid // TILE

    def scale_rows(i, carry):
        m, r = i // tr, i % tr
        at = pl.ds(pl.multiple_of(r * TILE, TILE), TILE)
        for j in range(tc):
            power = lax.shift_left(jnp.int32(1), exps_ref[m, r, j] + 15)
            factor = power.astype(F32) * (2.0 ** -15)
            cols = slice(j * TILE, (j + 1) * TILE)
            w[m, at, cols] = (w[m, at, cols].astype(F32) * factor).astype(BF)
        return carry

    lax.fori_loop(0, 3 * tr, scale_rows, 0)

    relays = []
    for k in range(1, pairs):
        pend[k].wait_recv()
        f = 2 * lax.rem(z - k + pairs, pairs) + core
        relays.append(send(slabs.at[f], slabs.at[f], s3_send.at[k], s3_recv.at[k], p, partner))
    pend[0].wait_recv()
    for copy in relays:
        copy.wait_recv()

    src, dst = iota((2 * rows, n_ex * 8), 1), iota((2 * rows, n_ex * 8), 0)
    kind, rest = dst // rows, dst % rows
    pick = jnp.where(
        src == (rest // CAP) * 8 + kind * CAP + rest % CAP, 1.0, 0.0
    ).astype(BF)
    got = [mm(pick, slabs[:, g].reshape(n_ex * 8, depth)) for g in range(n_dp)]
    xs = [
        jnp.concatenate([v[i * rows:(i + 1) * rows] for v in got], axis=0) for i in range(2)
    ]
    for i in range(2):
        x[i] = xs[i].astype(BF)

    sent = []
    for c in range(n_chunk):
        cols = slice(c * chunk, (c + 1) * chunk)
        for m in range(3):
            val = mm(x[m // 2], w[m, :, cols]).astype(F32)
            for g in range(n_dp):
                part_out[c, g, m] = val[g * rows:(g + 1) * rows].astype(BF)
        line = []
        for k in range(1, n_dp):
            q = lax.rem(p + k, n_dp)
            line.append(send(
                part_out.at[c, q], part_in.at[c, k], rs_send.at[c, k], rs_recv.at[c, k], q, e
            ))
        sent.append(line)

    for i in range(2):
        xt_ref[i] = x[i].astype(F32).T.astype(BF)

    shared = []
    for c in range(n_chunk):
        total = [part_out[c, p, m].astype(F32) for m in range(3)]
        for k in range(1, n_dp):
            sent[c][k - 1].wait_recv()
            total = [total[m] + part_in[c, k, m].astype(F32) for m in range(3)]
        gate, up, down = total
        sig = jax.nn.sigmoid(gate)
        act = gate * sig
        acts[c, p, 0] = (down * up * sig * (1.0 + gate * (1.0 - sig))).astype(BF)
        acts[c, p, 1] = (down * act).astype(BF)
        acts[c, p, 2] = (act * up).astype(BF)
        line = []
        for k in range(1, n_dp):
            q = lax.rem(p + k, n_dp)
            line.append(send(
                acts.at[c, p], acts.at[c, p], ag_send.at[c, k], ag_recv.at[c, k], q, e
            ))
        shared.append(line)

    for c in range(n_chunk):
        cols = slice(c * chunk, (c + 1) * chunk)
        for copy in shared[c]:
            copy.wait_recv()
        full = []
        for m in range(3):
            val = jnp.concatenate(
                [acts[c, g, m].astype(F32) for g in range(n_dp)], axis=0
            ).astype(BF)
            act_ref[m, :, cols] = val
            full.append(val)
        part = mm(full[0], w[0, :, cols], 1, 1) + mm(full[1], w[1, :, cols], 1, 1)
        if c == 0:
            acc[...] = part
        else:
            acc[...] += part

    pad = n_dp * 4
    summed = acc[...].astype(BF)
    batch = min(n_ex, 8)
    for b in range(n_ex // batch):
        shape = (batch * pad, n_dp * rows)
        to, frm = iota(shape, 0), iota(shape, 1)
        f, g, c = to // pad + b * batch, (to % pad) // 4, to % 4
        choose = jnp.where(
            (c < CAP) & (frm == g * rows + f * CAP + c), 1.0, 0.0
        ).astype(BF)
        val = mm(choose, summed).astype(BF)
        for j in range(batch):
            back_out[b * batch + j] = val[j * pad:(j + 1) * pad]
    back = []
    for k in range(1, n_ex):
        f = lax.rem(e + k, n_ex)
        back.append(send(back_out.at[f], back_in.at[k], b1_send.at[k], b1_recv.at[k], p, f))
    total = back_out[e].astype(F32)
    for k in range(1, n_ex):
        back[k - 1].wait_recv()
        total = total + back_in[k].astype(F32)
    for g in range(n_dp):
        own_out[g] = total[g * 4:(g + 1) * 4].astype(BF)
    last = []
    for k in range(1, n_dp):
        q = lax.rem(p + k, n_dp)
        last.append(send(own_out.at[q], own_in.at[p], b2_send.at[k], b2_recv.at[k], q, e))
    own_in[p] = own_out[p]
    for copy in last:
        copy.wait_recv()
    for q in range(n_dp):
        ig_ref[:, q * depth:(q + 1) * depth] = mm(
            hit_in[:, :4].astype(BF), own_in[q]
        ).astype(BF)

    for copy in pend[: pairs] + relays + back + last:
        copy.wait_send()
    for line in sent + shared:
        for copy in line:
            copy.wait_send()


def grads_kernel(xt_ref, act_ref, out_ref):
    out_ref[0] = mm(xt_ref[0], act_ref[0])


def per_device(n_dp, n_ex, out_grad, layer_input, expert_ids, gate_prob, w_stack, scale_exps):
    tok, width = out_grad.shape
    _, depth, hid = w_stack.shape
    rows = n_ex * CAP
    total = n_dp * rows
    chunk = min(256, hid)
    n_chunk = hid // chunk
    pad = n_dp * 4
    vm = pl.BlockSpec(memory_space=pltpu.VMEM)
    dma = pltpu.SemaphoreType.DMA
    pairs = n_ex // 2
    xt, act, input_grad = pl.pallas_call(
        functools.partial(exchange_kernel, n_dp, n_ex, chunk),
        out_shape=(
            jax.ShapeDtypeStruct((2, depth, total), BF),
            jax.ShapeDtypeStruct((3, total, hid), BF),
            jax.ShapeDtypeStruct((tok, width), BF),
        ),
        in_specs=[
            vm, vm, vm, vm,
            pl.BlockSpec(memory_space=pltpu.SMEM),
            pl.BlockSpec(memory_space=pl.ANY),
        ],
        out_specs=(vm, vm, vm),
        scratch_shapes=[
            pltpu.VMEM((3, depth, hid), BF),
            pltpu.VMEM((n_dp, 8, depth), BF),
            pltpu.VMEM((n_ex, n_dp, 8, depth), BF),
            pltpu.VMEM((2, total, depth), BF),
            pltpu.VMEM((n_chunk, n_dp, 3, rows, chunk), BF),
            pltpu.VMEM((n_chunk, n_dp, 3, rows, chunk), BF),
            pltpu.VMEM((n_chunk, n_dp, 3, rows, chunk), BF),
            pltpu.VMEM((total, depth), F32),
            pltpu.VMEM((n_ex, pad, depth), BF),
            pltpu.VMEM((n_ex, pad, depth), BF),
            pltpu.VMEM((n_dp, 4, depth), BF),
            pltpu.VMEM((n_dp, 4, depth), BF),
            dma((3,)),
            dma((n_dp,)), dma((n_dp,)),
            dma((pairs,)), dma((pairs,)),
            dma((pairs,)), dma((pairs,)),
            dma((n_chunk, n_dp)), dma((n_chunk, n_dp)),
            dma((n_chunk, n_dp)), dma((n_chunk, n_dp)),
            dma((n_ex,)), dma((n_ex,)),
            dma((n_dp,)), dma((n_dp,)),
        ],
        compiler_params=pltpu.CompilerParams(
            collective_id=0, has_side_effects=True, vmem_limit_bytes=VMEM_LIMIT
        ),
    )(out_grad, layer_input, expert_ids, gate_prob, scale_exps, w_stack)
    wide = min(512, hid)
    weight_grads = pl.pallas_call(
        grads_kernel,
        grid=(3, hid // wide),
        in_specs=[
            pl.BlockSpec((1, depth, total), lambda m, c: (m // 2, 0, 0)),
            pl.BlockSpec((1, total, wide), lambda m, c: (m, 0, c)),
        ],
        out_specs=pl.BlockSpec((1, depth, wide), lambda m, c: (m, 0, c)),
        out_shape=jax.ShapeDtypeStruct((3, depth, hid), F32),
        compiler_params=pltpu.CompilerParams(vmem_limit_bytes=VMEM_LIMIT),
    )(xt, act)
    return input_grad, weight_grads


def solution(mesh):
    in_specs = (
        P(("dp", "expert"), None),
        P(("dp", "expert"), None),
        P(("dp", "expert"), None),
        P(("dp", "expert"), None),
        P(None, "dp", "expert"),
        P(None, "dp", "expert"),
    )
    out_specs = (P(("dp", "expert"), None), P(None, "dp", "expert"))
    return jax.shard_map(
        functools.partial(per_device, mesh.shape["dp"], mesh.shape["expert"]),
        mesh=mesh, in_specs=in_specs, out_specs=out_specs, check_vma=False,
    )
```

```python
import functools

import jax
import jax.numpy as jnp
from jax import lax
from jax.experimental import pallas as pl
from jax.experimental.pallas import tpu as pltpu
from jax.sharding import PartitionSpec as P

TILE = 128
CAP = 3
DIRECT = 64
TALL = 256
BF = jnp.bfloat16
F32 = jnp.float32
VMEM_LIMIT = 60 * 1024 * 1024


def iota(shape, dim):
    return lax.broadcasted_iota(jnp.int32, shape, dim)


def mm(a, b, ca=1, cb=0):
    return lax.dot_general(a, b, (((ca,), (cb,)), ((), ())), preferred_element_type=F32)


def exchange_kernel(
    n_dp, n_ex, chunk,
    og_ref, li_ref, ids_ref, prob_ref, exps_ref, w_hbm,
    xt_ref, act_ref, ig_ref,
    w, slab_out, slabs, x, part_out, part_in, acts, hids, acc, back_out, back_in, own_out, own_in,
    w_sem, s1_send, s1_recv, s2_send, s2_recv, s3_send, s3_recv, rs_send, rs_recv,
    ag_send, ag_recv, hg_send, hg_recv, b1_send, b1_recv, b2_send, b2_recv,
):
    p, e = lax.axis_index("dp"), lax.axis_index("expert")
    tok, width = og_ref.shape
    _, depth, hid = w.shape
    rows = n_ex * CAP
    n_chunk = hid // chunk
    pairs = n_ex // 2
    z, core = e // 2, e % 2
    partner = 2 * z + 1 - core

    def send(src, dst, ssem, rsem, q, f):
        copy = pltpu.make_async_remote_copy(
            src_ref=src, dst_ref=dst, send_sem=ssem, recv_sem=rsem,
            device_id=(q, f), device_id_type=pl.DeviceIdType.MESH,
        )
        copy.start()
        return copy

    w_copies = [
        pltpu.make_async_copy(w_hbm.at[m], w.at[m], w_sem.at[m]) for m in range(3)
    ]
    for copy in w_copies:
        copy.start()

    barrier = pltpu.get_barrier_semaphore()
    for k in range(1, n_dp):
        pl.semaphore_signal(
            barrier, inc=1, device_id=(lax.rem(p + k, n_dp), e),
            device_id_type=pl.DeviceIdType.MESH,
        )
    for k in range(1, n_ex):
        pl.semaphore_signal(
            barrier, inc=1, device_id=(p, lax.rem(e + k, n_ex)),
            device_id_type=pl.DeviceIdType.MESH,
        )

    routed = ids_ref[...] == 0
    mask = jnp.max(routed.astype(F32), axis=0, keepdims=True)
    prob = jnp.sum(jnp.where(routed, prob_ref[...], 0.0), axis=0, keepdims=True)
    earlier = (iota((tok, tok), 0) <= iota((tok, tok), 1)).astype(BF)
    place = mm(jnp.broadcast_to(mask, (8, tok)).astype(BF), earlier) - 1.0
    mask_tall = jnp.broadcast_to(mask, (8, tok)) > 0.5
    row = iota((8, tok), 0).astype(F32)
    hit_in = jnp.where((place == row) & (row < CAP) & mask_tall, 1.0, 0.0)
    hit_gr = jnp.where((place + CAP == row) & (row >= CAP) & mask_tall, 1.0, 0.0)
    row_prob = jnp.sum(hit_gr * prob, axis=1, keepdims=True)
    slots = (
        mm(hit_in.astype(BF), li_ref[...]) + row_prob * mm(hit_gr.astype(BF), og_ref[...])
    ).astype(BF)
    for q in range(n_dp):
        slab_out[q] = slots[:, q * depth:(q + 1) * depth]
    pl.semaphore_wait(barrier, n_dp - 1 + n_ex - 1)

    pend = []
    for k in range(1, n_dp):
        q = lax.rem(p + k, n_dp)
        pend.append(send(slab_out.at[q], slabs.at[e, p], s1_send.at[k], s1_recv.at[k], q, e))
    slabs[e, p] = slab_out[p]
    for copy in pend:
        copy.wait()

    pend = [send(slabs.at[e], slabs.at[e], s2_send.at[0], s2_recv.at[0], p, partner)]
    for k in range(1, pairs):
        f = 2 * lax.rem(z + k, pairs) + core
        pend.append(send(slabs.at[e], slabs.at[e], s2_send.at[k], s2_recv.at[k], p, f))

    for copy in w_copies:
        copy.wait()
    tr, tc = depth // TILE, hid // TILE

    def scale_rows(i, carry):
        m, r = i // tr, i % tr
        at = pl.ds(pl.multiple_of(r * TILE, TILE), TILE)
        for j in range(tc):
            power = lax.shift_left(jnp.int32(1), exps_ref[m, r, j] + 15)
            factor = power.astype(F32) * (2.0 ** -15)
            cols = slice(j * TILE, (j + 1) * TILE)
            w[m, at, cols] = (w[m, at, cols].astype(F32) * factor).astype(BF)
        return carry

    lax.fori_loop(0, 3 * tr, scale_rows, 0)

    relays = []
    for k in range(1, pairs):
        pend[k].wait_recv()
        f = 2 * lax.rem(z - k + pairs, pairs) + core
        relays.append(send(slabs.at[f], slabs.at[f], s3_send.at[k], s3_recv.at[k], p, partner))
    pend[0].wait_recv()
    for copy in relays:
        copy.wait_recv()

    src, dst = iota((2 * rows, n_ex * 8), 1), iota((2 * rows, n_ex * 8), 0)
    kind, rest = dst // rows, dst % rows
    pick = jnp.where(
        src == (rest // CAP) * 8 + kind * CAP + rest % CAP, 1.0, 0.0
    ).astype(BF)
    got = [mm(pick, slabs[:, g].reshape(n_ex * 8, depth)) for g in range(n_dp)]
    xs = [
        jnp.concatenate([v[i * rows:(i + 1) * rows] for v in got], axis=0) for i in range(2)
    ]
    for i in range(2):
        x[i] = xs[i].astype(BF)

    sent = []
    for c in range(n_chunk):
        cols = slice(c * chunk, (c + 1) * chunk)
        for m in range(3):
            val = mm(x[m // 2], w[m, :, cols]).astype(F32)
            for g in range(n_dp):
                part_out[c, g, m] = val[g * rows:(g + 1) * rows].astype(BF)
        line = []
        for k in range(1, n_dp):
            q = lax.rem(p + k, n_dp)
            line.append(send(
                part_out.at[c, q], part_in.at[c, k], rs_send.at[c, k], rs_recv.at[c, k], q, e
            ))
        sent.append(line)

    for i in range(2):
        xt_ref[i] = x[i].astype(F32).T.astype(BF)

    shared = []
    for c in range(n_chunk):
        total = [part_out[c, p, m].astype(F32) for m in range(3)]
        for k in range(1, n_dp):
            sent[c][k - 1].wait_recv()
            total = [total[m] + part_in[c, k, m].astype(F32) for m in range(3)]
        gate, up, down = total
        sig = jax.nn.sigmoid(gate)
        act = gate * sig
        acts[c, p, 0] = (down * up * sig * (1.0 + gate * (1.0 - sig))).astype(BF)
        acts[c, p, 1] = (down * act).astype(BF)
        hids[c, p] = (act * up).astype(BF)
        line = []
        for k in range(1, n_dp):
            q = lax.rem(p + k, n_dp)
            line.append(send(
                acts.at[c, p], acts.at[c, p], ag_send.at[c, k], ag_recv.at[c, k], q, e
            ))
        shared.append(line)

    late = []
    for c in range(n_chunk):
        for k in range(1, n_dp):
            q = lax.rem(p + k, n_dp)
            late.append(send(
                hids.at[c, p], hids.at[c, p], hg_send.at[c, k], hg_recv.at[c, k], q, e
            ))

    for c in range(n_chunk):
        cols = slice(c * chunk, (c + 1) * chunk)
        for copy in shared[c]:
            copy.wait_recv()
        full = []
        for m in range(2):
            val = jnp.concatenate(
                [acts[c, g, m].astype(F32) for g in range(n_dp)], axis=0
            ).astype(BF)
            act_ref[m, :, cols] = val
            full.append(val)
        part = mm(full[0], w[0, :, cols], 1, 1) + mm(full[1], w[1, :, cols], 1, 1)
        if c == 0:
            acc[...] = part
        else:
            acc[...] += part

    pad = n_dp * 4
    summed = acc[...].astype(BF)
    batch = min(n_ex, 8)
    for b in range(n_ex // batch):
        shape = (batch * pad, n_dp * rows)
        to, frm = iota(shape, 0), iota(shape, 1)
        f, g, c = to // pad + b * batch, (to % pad) // 4, to % 4
        choose = jnp.where(
            (c < CAP) & (frm == g * rows + f * CAP + c), 1.0, 0.0
        ).astype(BF)
        val = mm(choose, summed)
        for j in range(batch):
            for g in range(n_dp):
                at = j * pad + g * 4
                back_out[b * batch + j, g] = val[at:at + 4].astype(BF)
    back, last = [], []
    if n_dp * n_ex <= DIRECT:
        for kf in range(n_ex - 1, -1, -1):
            for kq in range(n_dp - 1, -1, -1):
                if kq or kf:
                    q, f = lax.rem(p + kq, n_dp), lax.rem(e + kf, n_ex)
                    back.append(send(
                        back_out.at[f, q], back_in.at[e, p],
                        b1_send.at[kf, kq], b1_recv.at[kf, kq], q, f,
                    ))
        back_in[e, p] = back_out[e, p]
        for copy in late:
            copy.wait_recv()
        for c in range(n_chunk):
            act_ref[2, :, c * chunk:(c + 1) * chunk] = jnp.concatenate(
                [hids[c, g].astype(F32) for g in range(n_dp)], axis=0
            ).astype(BF)
        for copy in back:
            copy.wait_recv()
        for q in range(n_dp):
            total = back_in[0, q].astype(F32)
            for f in range(1, n_ex):
                total = total + back_in[f, q].astype(F32)
            own_in[q] = total.astype(BF)
    else:
        for k in range(1, n_ex):
            f = lax.rem(e + k, n_ex)
            back.append(send(back_out.at[f], back_in.at[k], b1_send.at[k, 0], b1_recv.at[k, 0], p, f))
        total = [back_out[e, g].astype(F32) for g in range(n_dp)]
        for k in range(1, n_ex):
            back[k - 1].wait_recv()
            total = [total[g] + back_in[k, g].astype(F32) for g in range(n_dp)]
        for g in range(n_dp):
            own_out[g] = total[g].astype(BF)
        for k in range(1, n_dp):
            q = lax.rem(p + k, n_dp)
            last.append(send(own_out.at[q], own_in.at[p], b2_send.at[k], b2_recv.at[k], q, e))
        own_in[p] = own_out[p]
        for copy in last:
            copy.wait_recv()
        for copy in late:
            copy.wait_recv()
        for c in range(n_chunk):
            act_ref[2, :, c * chunk:(c + 1) * chunk] = jnp.concatenate(
                [hids[c, g].astype(F32) for g in range(n_dp)], axis=0
            ).astype(BF)
    for q in range(n_dp):
        ig_ref[:, q * depth:(q + 1) * depth] = mm(
            hit_in[:4].astype(BF), own_in[q], 0, 0
        ).astype(BF)

    for copy in pend[:pairs] + relays + late + back + last:
        copy.wait_send()
    for line in sent + shared:
        for copy in line:
            copy.wait_send()


def grads_kernel(tall, xt_ref, act_ref, out_hbm, out, sems):
    _, depth, hid = out.shape
    steps = depth // tall
    copies = []
    for m in range(3):
        for r in range(steps):
            at = slice(r * tall, (r + 1) * tall)
            out[m, at, :] = mm(xt_ref[m // 2, at, :], act_ref[m])
            copy = pltpu.make_async_copy(
                out.at[m, at], out_hbm.at[m, at], sems.at[m * steps + r]
            )
            copy.start()
            copies.append(copy)
    for copy in copies:
        copy.wait()


def per_device(n_dp, n_ex, out_grad, layer_input, expert_ids, gate_prob, w_stack, scale_exps):
    tok, width = out_grad.shape
    _, depth, hid = w_stack.shape
    rows = n_ex * CAP
    total = n_dp * rows
    chunk = min(256, hid)
    n_chunk = hid // chunk
    n_last = n_dp if n_dp * n_ex <= DIRECT else 1
    vm = pl.BlockSpec(memory_space=pltpu.VMEM)
    dma = pltpu.SemaphoreType.DMA
    pairs = n_ex // 2
    xt, act, input_grad = pl.pallas_call(
        functools.partial(exchange_kernel, n_dp, n_ex, chunk),
        out_shape=(
            jax.ShapeDtypeStruct((2, depth, total), BF),
            jax.ShapeDtypeStruct((3, total, hid), BF),
            jax.ShapeDtypeStruct((tok, width), BF),
        ),
        in_specs=[
            vm, vm, vm, vm,
            pl.BlockSpec(memory_space=pltpu.SMEM),
            pl.BlockSpec(memory_space=pl.ANY),
        ],
        out_specs=(vm, vm, vm),
        scratch_shapes=[
            pltpu.VMEM((3, depth, hid), BF),
            pltpu.VMEM((n_dp, 8, depth), BF),
            pltpu.VMEM((n_ex, n_dp, 8, depth), BF),
            pltpu.VMEM((2, total, depth), BF),
            pltpu.VMEM((n_chunk, n_dp, 3, rows, chunk), BF),
            pltpu.VMEM((n_chunk, n_dp, 3, rows, chunk), BF),
            pltpu.VMEM((n_chunk, n_dp, 2, rows, chunk), BF),
            pltpu.VMEM((n_chunk, n_dp, rows, chunk), BF),
            pltpu.VMEM((total, depth), F32),
            pltpu.VMEM((n_ex, n_dp, 4, depth), BF),
            pltpu.VMEM((n_ex, n_dp, 4, depth), BF),
            pltpu.VMEM((n_dp, 4, depth), BF),
            pltpu.VMEM((n_dp, 4, depth), BF),
            dma((3,)),
            dma((n_dp,)), dma((n_dp,)),
            dma((pairs,)), dma((pairs,)),
            dma((pairs,)), dma((pairs,)),
            dma((n_chunk, n_dp)), dma((n_chunk, n_dp)),
            dma((n_chunk, n_dp)), dma((n_chunk, n_dp)),
            dma((n_chunk, n_dp)), dma((n_chunk, n_dp)),
            dma((n_ex, n_last)), dma((n_ex, n_last)),
            dma((n_dp,)), dma((n_dp,)),
        ],
        compiler_params=pltpu.CompilerParams(
            collective_id=0, has_side_effects=True, vmem_limit_bytes=VMEM_LIMIT
        ),
    )(out_grad, layer_input, expert_ids.T, gate_prob.T, scale_exps, w_stack)
    tall = min(TALL, depth)
    weight_grads = pl.pallas_call(
        functools.partial(grads_kernel, tall),
        in_specs=[vm, vm],
        out_specs=pl.BlockSpec(memory_space=pl.ANY),
        out_shape=jax.ShapeDtypeStruct((3, depth, hid), F32),
        scratch_shapes=[
            pltpu.VMEM((3, depth, hid), F32),
            dma((3 * (depth // tall),)),
        ],
        compiler_params=pltpu.CompilerParams(vmem_limit_bytes=VMEM_LIMIT),
    )(xt, act)
    return input_grad, weight_grads


def solution(mesh):
    in_specs = (
        P(("dp", "expert"), None),
        P(("dp", "expert"), None),
        P(("dp", "expert"), None),
        P(("dp", "expert"), None),
        P(None, "dp", "expert"),
        P(None, "dp", "expert"),
    )
    out_specs = (P(("dp", "expert"), None), P(None, "dp", "expert"))
    return jax.shard_map(
        functools.partial(per_device, mesh.shape["dp"], mesh.shape["expert"]),
        mesh=mesh, in_specs=in_specs, out_specs=out_specs, check_vma=False,
    )
```

```python
import functools

import jax
import jax.numpy as jnp
from jax import lax
from jax.experimental import pallas as pl
from jax.experimental.pallas import tpu as pltpu
from jax.sharding import PartitionSpec as P

TILE = 128
CAP = 3
DIRECT = 64
TALL = 256
BF = jnp.bfloat16
F32 = jnp.float32
VMEM_LIMIT = 60 * 1024 * 1024


def iota(shape, dim):
    return lax.broadcasted_iota(jnp.int32, shape, dim)


def mm(a, b, ca=1, cb=0):
    return lax.dot_general(a, b, (((ca,), (cb,)), ((), ())), preferred_element_type=F32)


def exchange_kernel(
    n_dp, n_ex, chunk,
    og_ref, li_ref, ids_ref, prob_ref, exps_ref, w_hbm,
    xt_ref, act_ref, ig_ref,
    w, slab_out, slabs, x, part_out, part_in, acts, hids, acc, back_out, back_in, own_out, own_in,
    w_sem, s1_send, s1_recv, s2_send, s2_recv, s3_send, s3_recv, rs_send, rs_recv,
    ag_send, ag_recv, hg_send, hg_recv, b1_send, b1_recv, b2_send, b2_recv,
):
    p, e = lax.axis_index("dp"), lax.axis_index("expert")
    tok, width = og_ref.shape
    _, depth, hid = w.shape
    rows = n_ex * CAP
    n_chunk = hid // chunk
    pairs = n_ex // 2
    z, core = e // 2, e % 2
    partner = 2 * z + 1 - core

    def send(src, dst, ssem, rsem, q, f):
        copy = pltpu.make_async_remote_copy(
            src_ref=src, dst_ref=dst, send_sem=ssem, recv_sem=rsem,
            device_id=(q, f), device_id_type=pl.DeviceIdType.MESH,
        )
        copy.start()
        return copy

    w_copies = [
        pltpu.make_async_copy(w_hbm.at[m], w.at[m], w_sem.at[m]) for m in range(3)
    ]
    for copy in w_copies:
        copy.start()

    barrier = pltpu.get_barrier_semaphore()
    for k in range(1, n_dp):
        pl.semaphore_signal(
            barrier, inc=1, device_id=(lax.rem(p + k, n_dp), e),
            device_id_type=pl.DeviceIdType.MESH,
        )
    for k in range(1, n_ex):
        pl.semaphore_signal(
            barrier, inc=1, device_id=(p, lax.rem(e + k, n_ex)),
            device_id_type=pl.DeviceIdType.MESH,
        )

    routed = ids_ref[...] == 0
    mask = jnp.max(routed.astype(F32), axis=0, keepdims=True)
    prob = jnp.sum(jnp.where(routed, prob_ref[...], 0.0), axis=0, keepdims=True)
    earlier = (iota((tok, tok), 0) <= iota((tok, tok), 1)).astype(BF)
    place = mm(jnp.broadcast_to(mask, (8, tok)).astype(BF), earlier) - 1.0
    mask_tall = jnp.broadcast_to(mask, (8, tok)) > 0.5
    row = iota((8, tok), 0).astype(F32)
    hit_in = jnp.where((place == row) & (row < CAP) & mask_tall, 1.0, 0.0)
    hit_gr = jnp.where((place + CAP == row) & (row >= CAP) & mask_tall, 1.0, 0.0)
    row_prob = jnp.sum(hit_gr * prob, axis=1, keepdims=True)
    slots = (
        mm(hit_in.astype(BF), li_ref[...]) + row_prob * mm(hit_gr.astype(BF), og_ref[...])
    ).astype(BF)
    for q in range(n_dp):
        slab_out[q] = slots[:, q * depth:(q + 1) * depth]
    pl.semaphore_wait(barrier, n_dp - 1 + n_ex - 1)

    pend = []
    for k in range(1, n_dp):
        q = lax.rem(p + k, n_dp)
        pend.append(send(slab_out.at[q], slabs.at[e, p], s1_send.at[k], s1_recv.at[k], q, e))
    slabs[e, p] = slab_out[p]
    for copy in pend:
        copy.wait()

    pend = [send(slabs.at[e], slabs.at[e], s2_send.at[0], s2_recv.at[0], p, partner)]
    for k in range(1, pairs):
        f = 2 * lax.rem(z + k, pairs) + core
        pend.append(send(slabs.at[e], slabs.at[e], s2_send.at[k], s2_recv.at[k], p, f))

    for copy in w_copies:
        copy.wait()
    tr, tc = depth // TILE, hid // TILE

    def scale_rows(i, carry):
        m, r = i // tr, i % tr
        at = pl.ds(pl.multiple_of(r * TILE, TILE), TILE)
        for j in range(tc):
            power = lax.shift_left(jnp.int32(1), exps_ref[m, r, j] + 15)
            factor = power.astype(F32) * (2.0 ** -15)
            cols = slice(j * TILE, (j + 1) * TILE)
            w[m, at, cols] = (w[m, at, cols].astype(F32) * factor).astype(BF)
        return carry

    lax.fori_loop(0, 3 * tr, scale_rows, 0)

    relays = []
    for k in range(1, pairs):
        pend[k].wait_recv()
        f = 2 * lax.rem(z - k + pairs, pairs) + core
        relays.append(send(slabs.at[f], slabs.at[f], s3_send.at[k], s3_recv.at[k], p, partner))
    pend[0].wait_recv()
    for copy in relays:
        copy.wait_recv()

    src, dst = iota((2 * rows, n_ex * 8), 1), iota((2 * rows, n_ex * 8), 0)
    kind, rest = dst // rows, dst % rows
    pick = jnp.where(
        src == (rest // CAP) * 8 + kind * CAP + rest % CAP, 1.0, 0.0
    ).astype(BF)
    got = [mm(pick, slabs[:, g].reshape(n_ex * 8, depth)) for g in range(n_dp)]
    xs = [
        jnp.concatenate([v[i * rows:(i + 1) * rows] for v in got], axis=0) for i in range(2)
    ]
    for i in range(2):
        x[i] = xs[i].astype(BF)

    sent = []
    for c in range(n_chunk):
        cols = slice(c * chunk, (c + 1) * chunk)
        for m in range(3):
            val = mm(x[m // 2], w[m, :, cols]).astype(F32)
            for g in range(n_dp):
                part_out[c, g, m] = val[g * rows:(g + 1) * rows].astype(BF)
        line = []
        for k in range(1, n_dp):
            q = lax.rem(p + k, n_dp)
            line.append(send(
                part_out.at[c, q], part_in.at[c, k], rs_send.at[c, k], rs_recv.at[c, k], q, e
            ))
        sent.append(line)

    for i in range(2):
        xt_ref[i] = x[i].astype(F32).T.astype(BF)

    shared = []
    for c in range(n_chunk):
        total = [part_out[c, p, m].astype(F32) for m in range(3)]
        for k in range(1, n_dp):
            sent[c][k - 1].wait_recv()
            total = [total[m] + part_in[c, k, m].astype(F32) for m in range(3)]
        gate, up, down = total
        sig = jax.nn.sigmoid(gate)
        act = gate * sig
        acts[c, p, 0] = (down * up * sig * (1.0 + gate * (1.0 - sig))).astype(BF)
        acts[c, p, 1] = (down * act).astype(BF)
        hids[c, p] = (act * up).astype(BF)
        line = []
        for k in range(1, n_dp):
            q = lax.rem(p + k, n_dp)
            line.append(send(
                acts.at[c, p], acts.at[c, p], ag_send.at[c, k], ag_recv.at[c, k], q, e
            ))
        shared.append(line)

    late = []
    for c in range(n_chunk):
        for k in range(1, n_dp):
            q = lax.rem(p + k, n_dp)
            late.append(send(
                hids.at[c, p], hids.at[c, p], hg_send.at[c, k], hg_recv.at[c, k], q, e
            ))

    for c in range(n_chunk):
        cols = slice(c * chunk, (c + 1) * chunk)
        for copy in shared[c]:
            copy.wait_recv()
        full = []
        for m in range(2):
            val = jnp.concatenate(
                [acts[c, g, m].astype(F32) for g in range(n_dp)], axis=0
            ).astype(BF)
            act_ref[m, :, cols] = val
            full.append(val)
        part = mm(full[0], w[0, :, cols], 1, 1) + mm(full[1], w[1, :, cols], 1, 1)
        if c == 0:
            acc[...] = part
        else:
            acc[...] += part

    pad = n_dp * 2
    half = depth // 2
    summed = acc[...].astype(BF)
    batch = min(n_ex, 8)
    for b in range(n_ex // batch):
        shape = (batch * pad, n_dp * rows)
        to, frm = iota(shape, 0), iota(shape, 1)
        f, g = to // pad + b * batch, (to % pad) // 2
        parts = []
        for t in range(CAP):
            piece = CAP * (to % 2) + t
            val = 0.0
            for h in range(2):
                choose = jnp.where(
                    (piece % 2 == h) & (frm == g * rows + f * CAP + piece // 2), 1.0, 0.0
                ).astype(BF)
                val = val + mm(choose, summed[:, h * half:(h + 1) * half])
            parts.append(val)
        val = jnp.concatenate(parts, axis=1)
        for j in range(batch):
            for g in range(n_dp):
                at = j * pad + g * 2
                back_out[b * batch + j, g] = val[at:at + 2].astype(BF)
    back, last = [], []
    if n_dp * n_ex <= DIRECT:
        for kf in range(n_ex - 1, -1, -1):
            for kq in range(n_dp - 1, -1, -1):
                if kq or kf:
                    q, f = lax.rem(p + kq, n_dp), lax.rem(e + kf, n_ex)
                    back.append(send(
                        back_out.at[f, q], back_in.at[e, p],
                        b1_send.at[kf, kq], b1_recv.at[kf, kq], q, f,
                    ))
        back_in[e, p] = back_out[e, p]
        for copy in late:
            copy.wait_recv()
        for c in range(n_chunk):
            act_ref[2, :, c * chunk:(c + 1) * chunk] = jnp.concatenate(
                [hids[c, g].astype(F32) for g in range(n_dp)], axis=0
            ).astype(BF)
        for copy in back:
            copy.wait_recv()
        for q in range(n_dp):
            total = back_in[0, q].astype(F32)
            for f in range(1, n_ex):
                total = total + back_in[f, q].astype(F32)
            own_in[q] = total.astype(BF)
    else:
        for k in range(1, n_ex):
            f = lax.rem(e + k, n_ex)
            back.append(send(back_out.at[f], back_in.at[k], b1_send.at[k, 0], b1_recv.at[k, 0], p, f))
        total = [back_out[e, g].astype(F32) for g in range(n_dp)]
        for k in range(1, n_ex):
            back[k - 1].wait_recv()
            total = [total[g] + back_in[k, g].astype(F32) for g in range(n_dp)]
        for g in range(n_dp):
            own_out[g] = total[g].astype(BF)
        for k in range(1, n_dp):
            q = lax.rem(p + k, n_dp)
            last.append(send(own_out.at[q], own_in.at[p], b2_send.at[k], b2_recv.at[k], q, e))
        own_in[p] = own_out[p]
        for copy in last:
            copy.wait_recv()
        for copy in late:
            copy.wait_recv()
        for c in range(n_chunk):
            act_ref[2, :, c * chunk:(c + 1) * chunk] = jnp.concatenate(
                [hids[c, g].astype(F32) for g in range(n_dp)], axis=0
            ).astype(BF)
    for q in range(n_dp):
        packed = own_in[q].astype(F32)
        halves = [
            packed[j // CAP:j // CAP + 1, (j % CAP) * half:(j % CAP + 1) * half]
            for j in range(2 * CAP)
        ]
        back_rows = jnp.concatenate(
            [jnp.concatenate(halves[2 * c:2 * c + 2], axis=1) for c in range(CAP)], axis=0
        ).astype(BF)
        ig_ref[:, q * depth:(q + 1) * depth] = mm(
            hit_in[:CAP].astype(BF), back_rows, 0, 0
        ).astype(BF)

    for copy in pend[:pairs] + relays + late + back + last:
        copy.wait_send()
    for line in sent + shared:
        for copy in line:
            copy.wait_send()


def grads_kernel(tall, xt_ref, act_ref, out_hbm, out, sems):
    _, depth, hid = out.shape
    steps = depth // tall
    copies = []
    for m in range(3):
        for r in range(steps):
            at = slice(r * tall, (r + 1) * tall)
            out[m, at, :] = mm(xt_ref[m // 2, at, :], act_ref[m])
            copy = pltpu.make_async_copy(
                out.at[m, at], out_hbm.at[m, at], sems.at[m * steps + r]
            )
            copy.start()
            copies.append(copy)
    for copy in copies:
        copy.wait()


def per_device(n_dp, n_ex, out_grad, layer_input, expert_ids, gate_prob, w_stack, scale_exps):
    tok, width = out_grad.shape
    _, depth, hid = w_stack.shape
    rows = n_ex * CAP
    total = n_dp * rows
    chunk = min(256, hid)
    n_chunk = hid // chunk
    n_last = n_dp if n_dp * n_ex <= DIRECT else 1
    vm = pl.BlockSpec(memory_space=pltpu.VMEM)
    dma = pltpu.SemaphoreType.DMA
    pairs = n_ex // 2
    xt, act, input_grad = pl.pallas_call(
        functools.partial(exchange_kernel, n_dp, n_ex, chunk),
        out_shape=(
            jax.ShapeDtypeStruct((2, depth, total), BF),
            jax.ShapeDtypeStruct((3, total, hid), BF),
            jax.ShapeDtypeStruct((tok, width), BF),
        ),
        in_specs=[
            vm, vm, vm, vm,
            pl.BlockSpec(memory_space=pltpu.SMEM),
            pl.BlockSpec(memory_space=pl.ANY),
        ],
        out_specs=(vm, vm, vm),
        scratch_shapes=[
            pltpu.VMEM((3, depth, hid), BF),
            pltpu.VMEM((n_dp, 8, depth), BF),
            pltpu.VMEM((n_ex, n_dp, 8, depth), BF),
            pltpu.VMEM((2, total, depth), BF),
            pltpu.VMEM((n_chunk, n_dp, 3, rows, chunk), BF),
            pltpu.VMEM((n_chunk, n_dp, 3, rows, chunk), BF),
            pltpu.VMEM((n_chunk, n_dp, 2, rows, chunk), BF),
            pltpu.VMEM((n_chunk, n_dp, rows, chunk), BF),
            pltpu.VMEM((total, depth), F32),
            pltpu.VMEM((n_ex, n_dp, 2, CAP * depth // 2), BF),
            pltpu.VMEM((n_ex, n_dp, 2, CAP * depth // 2), BF),
            pltpu.VMEM((n_dp, 2, CAP * depth // 2), BF),
            pltpu.VMEM((n_dp, 2, CAP * depth // 2), BF),
            dma((3,)),
            dma((n_dp,)), dma((n_dp,)),
            dma((pairs,)), dma((pairs,)),
            dma((pairs,)), dma((pairs,)),
            dma((n_chunk, n_dp)), dma((n_chunk, n_dp)),
            dma((n_chunk, n_dp)), dma((n_chunk, n_dp)),
            dma((n_chunk, n_dp)), dma((n_chunk, n_dp)),
            dma((n_ex, n_last)), dma((n_ex, n_last)),
            dma((n_dp,)), dma((n_dp,)),
        ],
        compiler_params=pltpu.CompilerParams(
            collective_id=0, has_side_effects=True, vmem_limit_bytes=VMEM_LIMIT
        ),
    )(out_grad, layer_input, expert_ids.T, gate_prob.T, scale_exps, w_stack)
    tall = min(TALL, depth)
    weight_grads = pl.pallas_call(
        functools.partial(grads_kernel, tall),
        in_specs=[vm, vm],
        out_specs=pl.BlockSpec(memory_space=pl.ANY),
        out_shape=jax.ShapeDtypeStruct((3, depth, hid), F32),
        scratch_shapes=[
            pltpu.VMEM((3, depth, hid), F32),
            dma((3 * (depth // tall),)),
        ],
        compiler_params=pltpu.CompilerParams(vmem_limit_bytes=VMEM_LIMIT),
    )(xt, act)
    return input_grad, weight_grads


def solution(mesh):
    in_specs = (
        P(("dp", "expert"), None),
        P(("dp", "expert"), None),
        P(("dp", "expert"), None),
        P(("dp", "expert"), None),
        P(None, "dp", "expert"),
        P(None, "dp", "expert"),
    )
    out_specs = (P(("dp", "expert"), None), P(None, "dp", "expert"))
    return jax.shard_map(
        functools.partial(per_device, mesh.shape["dp"], mesh.shape["expert"]),
        mesh=mesh, in_specs=in_specs, out_specs=out_specs, check_vma=False,
    )
```
